32 devices in a mesh: parts: 2 (over y), brick: 4 (over z), rep: 2 (over x), sub: 2 (over core).
Axes of the slice: x: 2, y: 2, z: 4, core: 2. Of those that a mesh axis runs over, the one named last changes fastest.
Arguments:
- fine_cells: int32 [5, 32768], P(None, ('parts', 'brick', 'rep', 'sub')), parts along dimension 1, may hold values from 0 to 511, as said below
- fine_exponent: float32 [32768], P(('parts', 'brick', 'rep', 'sub')), parts along dimension 0, may hold values from 0.05 to 0.6
- fine_charge: float32 [32768], P(('parts', 'brick', 'rep', 'sub')), parts along dimension 0, may hold values from -6 to 6
- fine_offset: float32 [3, 32768], P(None, ('parts', 'brick', 'rep', 'sub')), parts along dimension 1, may hold values from 0 to 1
- wide_cells: int32 [5, 4096], P(None, ('parts', 'brick', 'rep', 'sub')), parts along dimension 1, may hold values from 0 to 127, as said below
- wide_exponent: float32 [4096], P(('parts', 'brick', 'rep', 'sub')), parts along dimension 0, may hold values from 0.05 to 0.6
- wide_charge: float32 [4096], P(('parts', 'brick', 'rep', 'sub')), parts along dimension 0, may hold values from -6 to 6
- wide_offset: float32 [3, 4096], P(None, ('parts', 'brick', 'rep', 'sub')), parts along dimension 1, may hold values from 0 to 1
Outputs:
- finest_grid: float32 [256, 512, 512], P(('parts', 'brick'), ('rep', 'sub')), parts along dimension 0
- second_grid: float32 [128, 256, 256], P(('parts', 'brick'), ('rep', 'sub')), parts along dimension 0
- middle_grid: float32 [64, 16384], P('parts', 'brick'), parts along dimension 0
- coarse_grid: float32 [32, 4096], P('parts', 'brick'), parts along dimension 0
- coarsest_grid: float32 [16, 1024], P('parts', 'brick'), parts along dimension 0
The draws below stay inside these ranges and needn't reach their ends.
There are 2 independent parts, one for each index of `parts`. The reference program is written for one: setup_inputs(seed, part) draws one part's arguments, and reference() takes and returns one part's arrays. A program takes and returns all parts, laid end to end along the dimension named above; each array names one. Nothing has to cross between parts.
Inputs may be any that keep to these rules, and one draw needn't show every extreme that they name: `fine_cells`: column n is one fine Gaussian: row 0 its level L (0 or 1), row 1 its radius (1 to 4, equal to 4 on every 16th column), rows 2 to 4 its centre cell on level L's grid. The centre lies in the block of the device that holds column n: along the first dimension within that device's brick block of 128/2^L/4 cells, along the second within its block of 512/2^L/4 cells along rep+sub, anywhere along the third. `wide_cells`: column n is one wide Gaussian: row 0 its level L (2 to 4), row 1 its radius (1 to 4, equal to 4 on every 16th column), rows 2 to 4 its centre cell, anywhere on level L's grid.
All inputs are finite; a program needn't handle non-finite values.
Results may differ from the reference program's by a relative error of at most 0.0038.
Values sent between devices are 32-bit elements; how exact they have to be, the bound alone decides.
A program may use at most 64 MiB of HBM per device.

```python
import math
import jax
import jax.numpy as jnp
from jax import lax

GRID = 512
ROWS = 128
HALF = 4
FINE_DEV = 1024
WIDE_DEV = 128
FINE = 16384
WIDE = 2048
N_BRICK = 4
N_REP = 2
N_SUB = 2


def draw_fine_cells(key, part):
    slot_count = FINE_DEV * N_BRICK * N_REP * N_SUB
    slots = jnp.arange(slot_count, dtype=jnp.int32)
    device = slots // FINE_DEV
    columns = N_REP * N_SUB
    brick_index = device // columns
    column_index = device % columns
    level_row = (jax.random.randint(jax.random.fold_in(key, 1), (slot_count,), 0, 4) == 0).astype(jnp.int32)
    radius = jax.random.randint(jax.random.fold_in(key, 2), (slot_count,), 1, HALF + 1)
    radius = jnp.where(slots % 16 == 0, HALF, radius)
    row_tile = jnp.right_shift(jnp.int32(ROWS), level_row) // N_BRICK
    period = jnp.right_shift(jnp.int32(GRID), level_row)
    col_tile = period // columns
    picks = jax.random.randint(jax.random.fold_in(key, 3), (3, slot_count), 0, 1 << 20)
    first_cell = brick_index * row_tile + picks[0] % row_tile
    second_cell = column_index * col_tile + picks[1] % col_tile
    third_cell = picks[2] % period
    return jnp.stack([level_row, radius, first_cell, second_cell, third_cell]).astype(jnp.int32)


def draw_wide_cells(key, part):
    slot_count = WIDE_DEV * N_BRICK * N_REP * N_SUB
    slots = jnp.arange(slot_count, dtype=jnp.int32)
    choose = jax.random.randint(jax.random.fold_in(key, 5), (slot_count,), 0, 8)
    level_row = jnp.where(slots % 8 == 3, 4, jnp.where(choose < 2, 3, 2)).astype(jnp.int32)
    radius = jax.random.randint(jax.random.fold_in(key, 6), (slot_count,), 1, HALF + 1)
    radius = jnp.where(slots % 16 == 0, HALF, radius)
    rows_here = jnp.right_shift(jnp.int32(ROWS), level_row)
    period = jnp.right_shift(jnp.int32(GRID), level_row)
    picks = jax.random.randint(jax.random.fold_in(key, 7), (3, slot_count), 0, 1 << 20)
    first_cell = picks[0] % rows_here
    second_cell = picks[1] % period
    third_cell = picks[2] % period
    return jnp.stack([level_row, radius, first_cell, second_cell, third_cell]).astype(jnp.int32)


def block_levels(key, shape, shards, least, high):
    loudness, own = 1.0, jax.random.fold_in(key, 6)
    for axis_at, parts in shards:
        draws = jnp.exp(jax.random.uniform(jax.random.fold_in(own, axis_at), (parts,), jnp.float32, least / len(shards), high / len(shards)))
        loudness = loudness * jnp.repeat(draws, shape[axis_at] // parts).reshape([-1 if axis == axis_at else 1 for axis in range(len(shape))])
    return loudness


def bell_draw(rng, dims, scale, reach, cuts=(), kind=jnp.bfloat16):
    drawn = jax.random.normal(rng, dims, jnp.float32) * scale
    if len(cuts) > 0:
        drawn = block_levels(rng, dims, cuts, -0.22, 0.18) * drawn
    return jnp.clip(drawn, min=-reach, max=reach).astype(kind)


def setup_inputs(seed: int = 0, part: int = 0) -> dict:
    splits = jax.random.split(jax.random.key(seed), 9)
    own_keys = jax.random.split(jax.random.fold_in(splits[8], part), 9)
    return {
        "fine_cells": draw_fine_cells(jax.random.fold_in(jax.random.fold_in(splits[8], part), 71), part),
        "fine_exponent": jnp.clip(jnp.exp(math.log(0.6) - 2.4849067 * jax.random.uniform(own_keys[1], (FINE,), jnp.float32) ** block_levels(own_keys[1], (FINE,), ((0, 16),), -0.2, 0.2)), 0.05, 0.6),
        "fine_charge": bell_draw(own_keys[2], (FINE,), 1.0, 6.0, ((0, 16),), jnp.float32),
        "fine_offset": jnp.clip(1.0 * jax.random.uniform(own_keys[3], (3, FINE), jnp.float32) ** block_levels(own_keys[3], (3, FINE), ((1, 16),), -0.2, 0.2), 0.0, 1.0),
        "wide_cells": draw_wide_cells(jax.random.fold_in(jax.random.fold_in(splits[8], part), 71), part),
        "wide_exponent": jnp.clip(jnp.exp(math.log(0.6) - 2.4849067 * jax.random.uniform(own_keys[5], (WIDE,), jnp.float32) ** block_levels(own_keys[5], (WIDE,), ((0, 16),), -0.2, 0.2)), 0.05, 0.6),
        "wide_charge": bell_draw(own_keys[6], (WIDE,), 1.0, 6.0, ((0, 16),), jnp.float32),
        "wide_offset": jnp.clip(1.0 * jax.random.uniform(own_keys[7], (3, WIDE), jnp.float32) ** block_levels(own_keys[7], (3, WIDE), ((1, 16),), -0.2, 0.2), 0.0, 1.0),
    }


def one_factor(offsets, radius, exponent, centre_shift):
    inside = jnp.abs(offsets) <= radius[:, None]
    spread = offsets.astype(exponent.dtype) - centre_shift[:, None]
    return jnp.where(inside, jnp.exp(-exponent[:, None] * spread * spread), 0.0)


def deposit(slot_table, exponent, charge, offset, first_level, level_count):
    base_list = []
    grid_cells = 0
    for level_index in range(first_level, first_level + level_count):
        base_list.append(grid_cells)
        grid_cells += (ROWS >> level_index) * (GRID >> level_index) ** 2
    base_table = jnp.array(base_list, dtype=jnp.int32)
    slot_count = slot_table.shape[1]
    batch_size = math.gcd(slot_count, 4096)
    span_cells = jnp.arange(-HALF, HALF + 1, dtype=jnp.int32)
    span_count = 2 * HALF + 1

    def add_batch(flat_grid, batch_index):
        first_slot = (batch_index * batch_size).astype(jnp.int32)
        part_table = lax.dynamic_slice_in_dim(slot_table, first_slot, batch_size, 1)
        part_exponent = lax.dynamic_slice_in_dim(exponent, first_slot, batch_size, 0)
        part_charge = lax.dynamic_slice_in_dim(charge, first_slot, batch_size, 0)
        part_offset = lax.dynamic_slice_in_dim(offset, first_slot, batch_size, 1)
        level_row = part_table[0]
        radius = part_table[1]
        rows_here = jnp.right_shift(jnp.int32(ROWS), level_row)
        period = jnp.right_shift(jnp.int32(GRID), level_row)
        base_cell = base_table[level_row - first_level]
        offsets = jnp.broadcast_to(span_cells[None, :], (batch_size, span_count))
        row_place = part_table[2][:, None] + span_cells[None, :]
        col_place = jnp.mod(part_table[3][:, None] + span_cells[None, :], period[:, None])
        depth_place = jnp.mod(part_table[4][:, None] + span_cells[None, :], period[:, None])
        row_factor = one_factor(offsets, radius, part_exponent, part_offset[0])
        col_factor = one_factor(offsets, radius, part_exponent, part_offset[1])
        depth_factor = one_factor(offsets, radius, part_exponent, part_offset[2])
        plane_weight = ((part_charge[:, None] * row_factor)[:, :, None] * col_factor[:, None, :]).astype(jnp.bfloat16)
        depth_weight = depth_factor.astype(jnp.bfloat16)
        values = plane_weight.astype(jnp.float32)[:, :, :, None] * depth_weight.astype(jnp.float32)[:, None, None, :]
        period_four = period[:, None, None, None]
        flat_index = base_cell[:, None, None, None] + (row_place[:, :, None, None] * period_four + col_place[:, None, :, None]) * period_four + depth_place[:, None, None, :]
        inside_window = (row_place >= 0) & (row_place < rows_here[:, None])
        flat_index = jnp.where(inside_window[:, :, None, None], flat_index, grid_cells).astype(jnp.int32)
        flat_grid = flat_grid.at[flat_index.reshape(-1)].add(values.reshape(-1), mode="drop")
        return flat_grid, None

    start_grid = jnp.zeros((grid_cells,), jnp.float32)
    flat_grid, unused = lax.scan(add_batch, start_grid, jnp.arange(slot_count // batch_size, dtype=jnp.int32))
    return flat_grid


def reference(fine_cells, fine_exponent, fine_charge, fine_offset, wide_cells, wide_exponent, wide_charge, wide_offset):
    fine_flat = deposit(fine_cells, fine_exponent, fine_charge, fine_offset, 0, 2)
    level_zero = ROWS * GRID * GRID
    finest_grid = fine_flat[:level_zero].reshape(ROWS, GRID, GRID)
    second_grid = fine_flat[level_zero:].reshape(ROWS // 2, GRID // 2, GRID // 2)
    wide_flat = deposit(wide_cells, wide_exponent, wide_charge, wide_offset, 2, 3)
    outputs = []
    first_cell = 0
    for level_index in range(2, 5):
        rows_here = ROWS >> level_index
        period = GRID >> level_index
        outputs.append(wide_flat[first_cell:first_cell + rows_here * period * period].reshape(rows_here, period * period))
        first_cell += rows_here * period * period
    return (finest_grid, second_grid, outputs[0], outputs[1], outputs[2])
```

```python
import functools
import math

import jax
import jax.numpy as jnp
from jax import lax
from jax.experimental import pallas as pl
from jax.experimental.pallas import tpu as pltpu
from jax.sharding import PartitionSpec as P

GRID = 512
ROWS = 128
HALF = 4
SPILL = 384
WIDE_BLOCK = 1024
DIRECTIONS = [(i, j) for i in (-1, 0, 1) for j in (-1, 0, 1) if (i, j) != (0, 0)]
MESH = pl.DeviceIdType.MESH
F32 = jnp.float32
BF16 = jnp.bfloat16
I32 = jnp.int32
LOG2E = math.log2(math.e)
FLOATS = 5


def factor(cells, centre, radius, exponent, shift, period=None):
    reach = cells - (centre - radius)
    if period is not None:
        reach = reach & (period - 1)
        inside = reach <= 2 * radius
    else:
        inside = (reach >= 0) & (reach <= 2 * radius)
    spread = reach.astype(F32) - (radius.astype(F32) + shift)
    return jnp.where(inside, jnp.exp2((exponent * -LOG2E) * (spread * spread)), 0.0)


def halved(size, level):
    return lax.shift_right_logical(jnp.full(level.shape, size, I32), level)


def product(left, right):
    return lax.dot_general(left, right, (((1,), (1,)), ((), ())), preferred_element_type=F32)


def iota(shape):
    return lax.broadcasted_iota(I32, shape, 0)


def row_factor(cells, floats, rows, row_tile, row_block):
    level, radius = cells[0:1], cells[1:2]
    centre = cells[2:3] - row_block * halved(row_tile, level)
    shape = (rows, cells.shape[1])
    return floats[4:5] * factor(iota(shape), centre, radius, floats[3:4], floats[0:1])


def column_factor(cells, floats, columns, col_tile, col_block):
    level, radius = cells[0:1], cells[1:2]
    centre = cells[3:4] - col_block * halved(col_tile, level)
    shape = (columns, cells.shape[1])
    return factor(iota(shape), centre, radius, floats[3:4], floats[1:2], halved(GRID, level))


def depth_factor(cells, floats, width):
    level, radius = cells[0:1], cells[1:2]
    shape = (width, cells.shape[1])
    return factor(
        iota(shape), cells[4:5], radius, floats[3:4], floats[2:3], halved(GRID, level)
    ).astype(BF16)


def tiles(bricks, columns):
    row_tiles = [(ROWS >> level) // bricks for level in range(2)]
    col_tiles = [(GRID >> level) // columns for level in range(2)]
    periods = [GRID >> level for level in range(2)]
    return row_tiles, col_tiles, periods


def fine_factors(cells, floats, bricks, columns, brick, column):
    row_tiles, col_tiles, periods = tiles(bricks, columns)
    level = cells[0:1]
    row_weight = row_factor(cells, floats, row_tiles[0], row_tiles[0], brick)
    first = jnp.where(level == 0, row_weight, 0.0)
    second = jnp.where(level == 1, row_weight[0 : row_tiles[1]], 0.0)
    col = column_factor(cells, floats, col_tiles[0], col_tiles[0], column)
    return first, second, col, depth_factor(cells, floats, periods[0])


def local_kernel(bricks, reps, subs, *refs):
    fine_in, wide_in = refs[0:4], refs[4:8]
    near_i, near_f, wide_i, wide_f, part0, part1 = refs[8:14]
    own_i, own_f, own_wi, own_wf, depth, cols, row0, row1 = refs[14:22]
    fine_send, fine_recv, wide_send, wide_recv, own_sem, up_sem, down_sem = refs[22:]
    columns = reps * subs
    devices = bricks * columns
    brick = lax.axis_index("brick")
    column = lax.axis_index("rep") * subs + lax.axis_index("sub")
    me = brick * columns + column
    slots = own_i.shape[1]
    own_floats = own_f.at[:, 0:slots]
    wide_slots = wide_in[0].shape[1]
    row_tiles, col_tiles, periods = tiles(bricks, columns)
    parts = (part0, part1)
    rows = (row0, row1)

    def place(at_brick, at_column):
        return {"brick": at_brick, "rep": at_column // subs, "sub": at_column % subs}

    def at_column(step):
        return lax.rem(column + step, columns)

    def when_brick(step):
        return jnp.logical_and(brick + step >= 0, brick + step < bricks)

    barrier = pltpu.get_barrier_semaphore()

    def greet(step, first):
        @pl.when(when_brick(step))
        def _():
            @pl.loop(first, columns)
            def _(k):
                pl.semaphore_signal(
                    barrier, inc=1, device_id=place(brick + step, at_column(k)), device_id_type=MESH
                )

    greet(-1, 0)
    greet(0, 1)
    greet(1, 0)

    mine = pl.ds(pl.multiple_of(me * wide_slots, wide_slots), wide_slots)

    def fetches(source, whole_i, whole_f, first):
        pairs = [
            (source[0], whole_i),
            (source[3], whole_f.at[0:3]),
            (source[1], whole_f.at[3:4]),
            (source[2], whole_f.at[4:5]),
        ]
        return [
            pltpu.make_async_copy(a, b, own_sem.at[first + k]) for k, (a, b) in enumerate(pairs)
        ]

    own_wide = own_wf.at[:, 0:wide_slots]
    loads = fetches(wide_in, own_wi, own_wide, 0)
    loads += fetches(fine_in, own_i, own_floats, 4)
    for load in loads:
        load.start()
    for load in loads:
        load.wait()
    wide_i[:, mine] = own_wi[...]
    wide_f[:, mine] = own_wide[...]

    row0[...], row1[...], cols[...], depth[...] = fine_factors(
        own_i[...], own_floats[...], bricks, columns, brick, column
    )

    below = (brick > 0).astype(I32)
    above = (brick < bricks - 1).astype(I32)
    pl.semaphore_wait(barrier, columns - 1 + columns * (below + above))

    def wide_copy(to_brick, to_column, k):
        other = to_brick * columns + to_column
        return pltpu.make_async_remote_copy(
            src_ref=(own_wi, own_wide)[k],
            dst_ref=(wide_i, wide_f)[k].at[:, mine],
            send_sem=wide_send.at[other, k],
            recv_sem=wide_recv.at[me, k],
            device_id=place(to_brick, to_column),
            device_id_type=MESH,
        )

    def wide_to(to_brick, first):
        @pl.loop(first, columns)
        def _(step):
            for k in range(2):
                wide_copy(to_brick, at_column(step), k).start()

    def fine_copy(direction, k):
        up, across = DIRECTIONS[direction]
        slot = 7 - direction
        return pltpu.make_async_remote_copy(
            src_ref=(own_i, own_floats)[k],
            dst_ref=(near_i, near_f)[k].at[:, pl.ds(slot * slots, slots)],
            send_sem=fine_send.at[direction, k],
            recv_sem=fine_recv.at[slot, k],
            device_id=place(brick + up, at_column(across + columns)),
            device_id_type=MESH,
        )

    def token(step, sem):
        pl.semaphore_signal(sem, inc=1, device_id=place(brick + step, column), device_id_type=MESH)

    for step in (-1, 1):

        @pl.when(when_brick(step))
        def _():
            wide_to(brick + step, 0)

    wide_to(brick, 1)

    for direction in (1, 6, 0, 2, 5, 7, 3, 4):

        @pl.when(when_brick(DIRECTIONS[direction][0]))
        def _():
            for k in range(2):
                fine_copy(direction, k).start()

    @pl.when(brick >= 2)
    def _():
        pl.semaphore_wait(up_sem, 1)

    @pl.when(jnp.logical_and(brick >= 1, brick < bricks - 1))
    def _():
        token(1, up_sem)

    @pl.loop(0, jnp.maximum(brick - 1, 0))
    def _(to_brick):
        wide_to(to_brick, 0)

    def slab(level, first, per):
        weights = jnp.concatenate(
            [
                (rows[level][pl.ds(first + i, 1), :] * cols[0 : col_tiles[level], :]).astype(BF16)
                for i in range(per)
            ],
            0,
        )
        result = product(weights, depth[0 : periods[level], :])
        return result.reshape(per, col_tiles[level], periods[level])

    per1 = min(4, row_tiles[1])
    per0 = min(4, row_tiles[0])

    @pl.loop(0, row_tiles[1] // per1)
    def _(i):
        parts[1][pl.ds(i * per1, per1)] = slab(1, i * per1, per1)

    half0 = row_tiles[0] // per0 // 2

    @pl.loop(0, half0)
    def _(i):
        parts[0][pl.ds(i * per0, per0)] = slab(0, i * per0, per0)

    @pl.when(brick < bricks - 2)
    def _():
        pl.semaphore_wait(down_sem, 1)

    @pl.when(jnp.logical_and(brick >= 1, brick < bricks - 1))
    def _():
        token(-1, down_sem)

    @pl.loop(jnp.minimum(brick + 2, bricks), bricks)
    def _(to_brick):
        wide_to(to_brick, 0)

    @pl.loop(half0, row_tiles[0] // per0)
    def _(i):
        parts[0][pl.ds(i * per0, per0)] = slab(0, i * per0, per0)

    for direction in range(8):

        @pl.when(when_brick(DIRECTIONS[direction][0]))
        def _():
            for k in range(2):
                fine_copy(direction, k).wait_send()
                spot = (near_i, near_f)[k].at[:, pl.ds(direction * slots, slots)]
                own = (own_i, own_floats)[k]
                pltpu.make_async_copy(own, spot, fine_recv.at[direction, k]).wait()

    @pl.loop(1, devices)
    def _(step):
        at = lax.rem(me + step, devices)
        spot = pl.ds(pl.multiple_of(at * wide_slots, wide_slots), wide_slots)
        for k in range(2):
            wide_copy(at // columns, lax.rem(at, columns), k).wait_send()
            ref = (wide_i, wide_f)[k].at[:, spot]
            pltpu.make_async_copy((own_wi, own_wide)[k], ref, wide_recv.at[at, k]).wait()


def local_part(mesh_shape, fine, wide):
    bricks, reps, subs = (mesh_shape[name] for name in ("brick", "rep", "sub"))
    columns = reps * subs
    devices = bricks * columns
    row_tiles, col_tiles, periods = tiles(bricks, columns)
    slots, wide_slots = fine[0].shape[1], wide[0].shape[1]
    outs = [
        pltpu.VMEM((5, 8 * slots), I32),
        pltpu.VMEM((8, 8 * slots), F32),
        pltpu.VMEM((5, devices * wide_slots), I32),
        pltpu.VMEM((8, devices * wide_slots), F32),
    ] + [pltpu.VMEM((row_tiles[k], col_tiles[k], periods[k]), F32) for k in range(2)]
    return pl.pallas_call(
        functools.partial(local_kernel, bricks, reps, subs),
        out_shape=outs,
        in_specs=[pl.BlockSpec(memory_space=pltpu.HBM)] * 8,
        out_specs=[pl.BlockSpec(memory_space=pltpu.VMEM)] * 6,
        scratch_shapes=[
            pltpu.VMEM((5, slots), I32),
            pltpu.VMEM((8, slots + 128), F32),
            pltpu.VMEM((5, wide_slots), I32),
            pltpu.VMEM((8, wide_slots + 128), F32),
            pltpu.VMEM((periods[0], slots), BF16),
            pltpu.VMEM((col_tiles[0], slots), F32),
            pltpu.VMEM((row_tiles[0], slots), F32),
            pltpu.VMEM((row_tiles[1], slots), F32),
            pltpu.SemaphoreType.DMA((8, 2)),
            pltpu.SemaphoreType.DMA((8, 2)),
            pltpu.SemaphoreType.DMA((devices, 2)),
            pltpu.SemaphoreType.DMA((devices, 2)),
            pltpu.SemaphoreType.DMA((8,)),
            pltpu.SemaphoreType.REGULAR,
            pltpu.SemaphoreType.REGULAR,
        ],
        compiler_params=pltpu.CompilerParams(
            collective_id=0, has_side_effects=True, vmem_limit_bytes=30 * 1024 * 1024
        ),
        name="local_part",
    )(*[pltpu.with_memory_space_constraint(a, pltpu.HBM) for a in (*fine, *wide)])


def finish_kernel(bricks, columns, subs, slots, wide_block, *refs):
    near_i, near_f, wide_i, wide_f, part0, part1 = refs[0:6]
    out0, out1, out2, out3, out4 = refs[6:11]
    depth, cols, row0, row1, spread_at, chunks, sems = refs[11:]
    brick = lax.axis_index("brick")
    column = lax.axis_index("rep") * subs + lax.axis_index("sub")
    row_tiles, col_tiles, periods = tiles(bricks, columns)
    parts, outs, rows = (part0, part1), (out0, out1), (row0, row1)
    edge = 2 * HALF
    inner = [row_tiles[k] > 2 * HALF and col_tiles[k] > 2 * edge for k in range(2)]

    def copy_out(level, row, height, col, width, sem):
        spot = (pl.ds(row, height), pl.ds(col, width))
        return pltpu.make_async_copy(parts[level].at[spot], outs[level].at[spot], sems.at[sem])

    early, late = [], []
    for level in range(2):
        tall, wide_cols = row_tiles[level], col_tiles[level]
        base = 8 * level
        if inner[level]:
            height = tall - 2 * HALF
            early.append(copy_out(level, HALF, height, edge, wide_cols - 2 * edge, base))
            late.append(copy_out(level, HALF, height, 0, edge, base + 1))
            late.append(copy_out(level, HALF, height, wide_cols - edge, edge, base + 2))
            late.append(copy_out(level, 0, HALF, 0, wide_cols, base + 3))
            late.append(copy_out(level, tall - HALF, HALF, 0, wide_cols, base + 4))
        else:
            late.append(copy_out(level, 0, tall, 0, wide_cols, base + 1))
    for copy in early:
        copy.start()

    def gather_spill(chunk):
        ints = jnp.zeros((48, SPILL), F32)
        at = lax.broadcasted_iota(I32, (SPILL, slots), 0).astype(F32) + (chunk * SPILL).astype(F32)
        for s in range(8):
            where_to = spread_at[s : s + 1, :]
            span = pl.ds(s * slots, slots)
            pad = jnp.zeros((16 - 5 - FLOATS, slots), F32)
            table = jnp.concatenate([near_i[:, span].astype(F32), near_f[0:FLOATS, span], pad], 0)
            values = jnp.where(where_to >= 0, table, 0.0)
            high = values.astype(BF16)
            rest = values - high.astype(F32)
            middle = rest.astype(BF16)
            low = (rest - middle.astype(F32)).astype(BF16)
            pieces = jnp.concatenate([high, middle, low], 0)
            chosen = jnp.where(where_to == at, 1.0, 0.0).astype(BF16)
            ints += product(pieces, chosen)
        total = ints[0:16] + ints[16:32] + ints[32:48]
        return total[0:5].astype(I32), total[5 : 5 + FLOATS]

    def spill_places():
        def lined(k):
            return jnp.concatenate(
                [near_i[k : k + 1, s * slots : (s + 1) * slots] for s in range(8)], 0
            )

        level, radius, c0, c1 = (lined(k) for k in range(4))
        first = level == 0
        row_tile = jnp.where(first, row_tiles[0], row_tiles[1])
        col_tile = jnp.where(first, col_tiles[0], col_tiles[1])
        period = jnp.where(first, periods[0], periods[1])
        across = c0 - brick * row_tile
        along = ((c1 - column * col_tile + period // 2) & (period - 1)) - period // 2
        line = lax.broadcasted_iota(I32, level.shape, 0)
        up = jnp.where(line < 3, -1, jnp.where(line < 5, 0, 1)) + brick
        keep = (up >= 0) & (up < bricks)
        keep &= (across >= -radius) & (across < row_tile + radius)
        wrap = along + period
        keep &= ((along >= -radius) & (along < col_tile + radius)) | (wrap < col_tile + radius)
        keep = jnp.where(keep, 1.0, 0.0)
        count = slots // 128
        piled = jnp.concatenate([keep[:, i * 128 : (i + 1) * 128] for i in range(count)], 0)
        height = piled.shape[0]
        upper = lax.broadcasted_iota(I32, (128, 128), 0) <= lax.broadcasted_iota(I32, (128, 128), 1)
        within = jnp.dot(
            piled.astype(BF16), jnp.where(upper, 1.0, 0.0).astype(BF16), preferred_element_type=F32
        )
        sums = jnp.broadcast_to(within[:, 127:128], (height, 128))
        lower = lax.broadcasted_iota(I32, (height, height), 0) > lax.broadcasted_iota(
            I32, (height, height), 1
        )
        before = jnp.dot(
            jnp.where(lower, 1.0, 0.0).astype(BF16), sums.astype(BF16), preferred_element_type=F32
        )
        at = jnp.where(piled > 0.0, before + within - 1.0, -1.0)
        for i in range(count):
            spread_at[:, i * 128 : (i + 1) * 128] = at[i * 8 : (i + 1) * 8]
        chunks[0] = (jnp.max(at).astype(I32) + SPILL) // SPILL

    def add_rows(level, row, height, col, width):
        weights = jnp.concatenate(
            [
                (rows[level][row + i : row + i + 1, :] * cols[col : col + width, :]).astype(BF16)
                for i in range(height)
            ],
            0,
        )
        result = product(weights, depth[0 : periods[level], :])
        spot = (slice(row, row + height), slice(col, col + width))
        parts[level][spot] += result.reshape(height, width, periods[level])

    def add_spill(chunk):
        cells, floats = gather_spill(chunk)
        row0[...], row1[...], cols[...], depth[...] = fine_factors(
            cells, floats, bricks, columns, brick, column
        )
        for level in range(2):
            tall, wide_cols = row_tiles[level], col_tiles[level]
            if inner[level]:
                for row in (0, tall - HALF):
                    add_rows(level, row, HALF, 0, wide_cols)
                for row in range(HALF, tall - HALF, 8):
                    height = min(8, tall - HALF - row)
                    for col in (0, wide_cols - edge):
                        add_rows(level, row, height, col, edge)
            else:
                for row in range(0, tall, HALF):
                    add_rows(level, row, min(HALF, tall - row), 0, wide_cols)

    spill_places()
    add_spill(jnp.int32(0))

    @pl.loop(1, chunks[0])
    def _(chunk):
        add_spill(chunk)

    for copy in late:
        copy.start()

    def wide_part(part):
        span = pl.ds(pl.multiple_of(part * wide_block, wide_block), wide_block)
        cells, floats = wide_i[:, span], wide_f[0:FLOATS, span]
        share = (GRID >> 2) // bricks
        which = cells[0:1]
        row_weight = row_factor(cells, floats, ROWS >> 2, ROWS, 0)
        col = column_factor(cells, floats, share, GRID // bricks, brick)
        lanes = GRID >> 2
        depth_value = depth_factor(cells, floats, lanes)
        for level, out in ((2, out2), (3, out3), (4, out4)):
            period = GRID >> level
            height = ROWS >> level
            share = period // bricks
            group = min(share, 8)
            copies = lanes // period
            width = min(copies, group)
            own = jnp.where(which == level, row_weight[0:height], 0.0)
            lane = lax.broadcasted_iota(I32, (height, lanes), 1) // period
            for first in range(0, share, group):
                weights = jnp.concatenate(
                    [(own * col[i : i + 1]).astype(BF16) for i in range(first, first + group)], 0
                )
                result = product(weights, depth_value)
                for i in range(0, group, width):
                    piece = result[i * height : (i + 1) * height]
                    for j in range(1, width):
                        piece = jnp.where(
                            lane == j, result[(i + j) * height : (i + j + 1) * height], piece
                        )
                    start = (first + i) * period
                    out[:, start : start + width * period] += piece[:, 0 : width * period]

    for ref in (out2, out3, out4):
        ref[...] = jnp.zeros(ref.shape, F32)

    @pl.loop(0, wide_i.shape[1] // wide_block)
    def _(part):
        wide_part(part)

    for copy in early + late:
        copy.wait()


def finish(mesh_shape, slots, got):
    bricks, reps, subs = (mesh_shape[name] for name in ("brick", "rep", "sub"))
    columns = reps * subs
    row_tiles, col_tiles, periods = tiles(bricks, columns)
    block = min(WIDE_BLOCK, got[2].shape[1])
    shapes = [(row_tiles[level], col_tiles[level], periods[level]) for level in range(2)]
    shapes += [(ROWS >> level, (GRID >> level) ** 2 // bricks) for level in (2, 3, 4)]
    vmem, anywhere = pl.BlockSpec(memory_space=pltpu.VMEM), pl.BlockSpec(memory_space=pl.ANY)
    return pl.pallas_call(
        functools.partial(finish_kernel, bricks, columns, subs, slots, block),
        out_shape=[jax.ShapeDtypeStruct(shape, F32) for shape in shapes],
        in_specs=[vmem] * 6,
        out_specs=[anywhere] * 2 + [vmem] * 3,
        scratch_shapes=[
            pltpu.VMEM((periods[0], SPILL), BF16),
            pltpu.VMEM((col_tiles[0], SPILL), F32),
            pltpu.VMEM((row_tiles[0], SPILL), F32),
            pltpu.VMEM((row_tiles[1], SPILL), F32),
            pltpu.VMEM((8, slots), F32),
            pltpu.SMEM((1,), I32),
            pltpu.SemaphoreType.DMA((16,)),
        ],
        compiler_params=pltpu.CompilerParams(vmem_limit_bytes=30 * 1024 * 1024),
        name="finish",
    )(*got)


def solution(mesh):
    shape = dict(mesh.shape)

    def per_device(
        fine_cells,
        fine_exponent,
        fine_charge,
        fine_offset,
        wide_cells,
        wide_exponent,
        wide_charge,
        wide_offset,
    ):
        fine = (fine_cells, fine_exponent[None, :], fine_charge[None, :], fine_offset)
        wide = (wide_cells, wide_exponent[None, :], wide_charge[None, :], wide_offset)
        got = local_part(shape, fine, wide)
        return tuple(finish(shape, fine_cells.shape[1], got))

    split = P(("parts", "brick", "rep", "sub"))
    table = P(None, ("parts", "brick", "rep", "sub"))
    return jax.shard_map(
        per_device,
        mesh=mesh,
        in_specs=(table, split, split, table, table, split, split, table),
        out_specs=(
            P(("parts", "brick"), ("rep", "sub"), None),
            P(("parts", "brick"), ("rep", "sub"), None),
            P("parts", "brick"),
            P("parts", "brick"),
            P("parts", "brick"),
        ),
        check_vma=False,
    )
```

```python
import functools
import math

import jax
import jax.numpy as jnp
from jax import lax
from jax.experimental import pallas as pl
from jax.experimental.pallas import tpu as pltpu
from jax.sharding import PartitionSpec as P

GRID = 512
ROWS = 128
HALF = 4
SPILL = 256
WIDE_BLOCK = 1024
DIRECTIONS = [(i, j) for i in (-1, 0, 1) for j in (-1, 0, 1) if (i, j) != (0, 0)]
MESH = pl.DeviceIdType.MESH
F32 = jnp.float32
BF16 = jnp.bfloat16
I32 = jnp.int32
LOG2E = math.log2(math.e)
FLOATS = 5
LISTS = 512
CAPS = (16, 160, 16, 48, 48, 16, 160, 16)
STARTS = (320, 160, 336, 384, 432, 352, 0, 368)
LANES = 128


def factor(cells, centre, radius, exponent, shift, period=None):
    reach = cells - (centre - radius)
    if period is not None:
        reach = reach & (period - 1)
        inside = reach <= 2 * radius
    else:
        inside = (reach >= 0) & (reach <= 2 * radius)
    spread = reach.astype(F32) - (radius.astype(F32) + shift)
    return jnp.where(inside, jnp.exp2((exponent * -LOG2E) * (spread * spread)), 0.0)


def halved(size, level):
    return lax.shift_right_logical(jnp.full(level.shape, size, I32), level)


def product(left, right):
    return lax.dot_general(left, right, (((1,), (1,)), ((), ())), preferred_element_type=F32)


def iota(shape):
    return lax.broadcasted_iota(I32, shape, 0)


def row_factor(cells, floats, rows, row_tile, row_block):
    level, radius = cells[0:1], cells[1:2]
    centre = cells[2:3] - row_block * halved(row_tile, level)
    shape = (rows, cells.shape[1])
    return floats[4:5] * factor(iota(shape), centre, radius, floats[3:4], floats[0:1])


def column_factor(cells, floats, columns, col_tile, col_block):
    level, radius = cells[0:1], cells[1:2]
    centre = cells[3:4] - col_block * halved(col_tile, level)
    shape = (columns, cells.shape[1])
    return factor(iota(shape), centre, radius, floats[3:4], floats[1:2], halved(GRID, level))


def depth_factor(cells, floats, width):
    level, radius = cells[0:1], cells[1:2]
    shape = (width, cells.shape[1])
    return factor(
        iota(shape), cells[4:5], radius, floats[3:4], floats[2:3], halved(GRID, level)
    ).astype(BF16)


def tiles(bricks, columns):
    row_tiles = [(ROWS >> level) // bricks for level in range(2)]
    col_tiles = [(GRID >> level) // columns for level in range(2)]
    periods = [GRID >> level for level in range(2)]
    return row_tiles, col_tiles, periods


def fine_factors(cells, floats, bricks, columns, brick, column):
    row_tiles, col_tiles, periods = tiles(bricks, columns)
    level = cells[0:1]
    row_weight = row_factor(cells, floats, row_tiles[0], row_tiles[0], brick)
    first = jnp.where(level == 0, row_weight, 0.0)
    second = jnp.where(level == 1, row_weight[0 : row_tiles[1]], 0.0)
    col = column_factor(cells, floats, col_tiles[0], col_tiles[0], column)
    return first, second, col, depth_factor(cells, floats, periods[0])


def ranks(keep, by_row):
    count = keep.shape[1] // LANES
    piled = jnp.concatenate([keep[:, i * LANES : (i + 1) * LANES] for i in range(count)], 0)
    height = piled.shape[0]
    square = (LANES, LANES)
    upper = iota(square) <= lax.broadcasted_iota(I32, square, 1)
    within = jnp.dot(
        piled.astype(BF16), jnp.where(upper, 1.0, 0.0).astype(BF16), preferred_element_type=F32
    )
    sums = jnp.broadcast_to(within[:, LANES - 1 : LANES], piled.shape)
    square = (height, height)
    gap = iota(square) - lax.broadcasted_iota(I32, square, 1)
    lower = gap > 0
    if by_row:
        lower &= (gap & 7) == 0
    before = jnp.dot(
        jnp.where(lower, 1.0, 0.0).astype(BF16), sums.astype(BF16), preferred_element_type=F32
    )
    at = before + within - 1.0
    return jnp.concatenate([at[i * 8 : (i + 1) * 8] for i in range(count)], 1)


def gather(cells, floats, chosen):
    count = cells.shape[1]
    pad = jnp.zeros((16 - 5 - FLOATS, count), F32)
    values = jnp.concatenate([cells.astype(F32), floats, pad], 0)
    high = values.astype(BF16)
    rest = values - high.astype(F32)
    middle = rest.astype(BF16)
    low = (rest - middle.astype(F32)).astype(BF16)
    found = product(jnp.concatenate([high, middle, low], 0), chosen)
    return found[0:16] + found[16:32] + found[32:48]


def by_line(values, shape):
    line = iota(shape)
    out = jnp.full(shape, values[0], F32)
    for k in range(1, len(values)):
        out = jnp.where(line == k, float(values[k]), out)
    return out


def touched(up, across, row_tile, col_tile, low0, high0, low1, high1):
    along0 = {-1: low0 < 0, 0: None, 1: high0 >= row_tile}[up]
    along1 = {-1: low1 < 0, 0: None, 1: high1 >= col_tile}[across]
    if along0 is None:
        return along1
    return along0 if along1 is None else along0 & along1


def add_spill(parts, rows, cols, depth, row_tiles, col_tiles, periods):
    edge = 2 * HALF

    def add_rows(level, row, height, col, width):
        weights = jnp.concatenate(
            [
                (rows[level][row + i : row + i + 1, :] * cols[col : col + width, :]).astype(BF16)
                for i in range(height)
            ],
            0,
        )
        result = product(weights, depth[0 : periods[level], :])
        spot = (slice(row, row + height), slice(col, col + width))
        parts[level][spot] += result.reshape(height, width, periods[level])

    for level in range(2):
        tall, wide = row_tiles[level], col_tiles[level]
        if tall > 2 * HALF and wide > 2 * edge:
            for row in (0, tall - HALF):
                add_rows(level, row, HALF, 0, wide)
            for col in (0, wide - edge):
                add_rows(level, HALF, tall - 2 * HALF, col, edge)
        else:
            for row in range(0, tall, HALF):
                add_rows(level, row, min(HALF, tall - row), 0, wide)


def local_kernel(bricks, reps, subs, *refs):
    fine_in, wide_in = refs[0:4], refs[4:8]
    wide_i, wide_f, part0, part1, over = refs[8:13]
    own_i, own_f, own_wi, own_wf, depth, cols, row0, row1 = refs[13:21]
    list_i, list_f, near_i, near_f, depth2, cols2, row02, row12 = refs[21:29]
    fine_send, fine_recv, wide_send, wide_recv, own_sem, up_sem, down_sem = refs[29:]
    columns = reps * subs
    devices = bricks * columns
    brick = lax.axis_index("brick")
    column = lax.axis_index("rep") * subs + lax.axis_index("sub")
    me = brick * columns + column
    slots = own_i.shape[1]
    own_floats = own_f.at[:, 0:slots]
    wide_slots = wide_in[0].shape[1]
    row_tiles, col_tiles, periods = tiles(bricks, columns)
    parts = (part0, part1)
    rows = (row0, row1)

    def place(at_brick, at_column):
        return {"brick": at_brick, "rep": at_column // subs, "sub": at_column % subs}

    def at_column(step):
        return lax.rem(column + step, columns)

    def when_brick(step):
        return jnp.logical_and(brick + step >= 0, brick + step < bricks)

    barrier = pltpu.get_barrier_semaphore()

    def greet(step, first):
        @pl.when(when_brick(step))
        def _():
            @pl.loop(first, columns)
            def _(k):
                pl.semaphore_signal(
                    barrier, inc=1, device_id=place(brick + step, at_column(k)), device_id_type=MESH
                )

    greet(-1, 0)
    greet(0, 1)
    greet(1, 0)

    mine = pl.ds(pl.multiple_of(me * wide_slots, wide_slots), wide_slots)

    def fetches(source, whole_i, whole_f, first):
        pairs = [
            (source[0], whole_i),
            (source[3], whole_f.at[0:3]),
            (source[1], whole_f.at[3:4]),
            (source[2], whole_f.at[4:5]),
        ]
        return [
            pltpu.make_async_copy(a, b, own_sem.at[first + k]) for k, (a, b) in enumerate(pairs)
        ]

    own_wide = own_wf.at[:, 0:wide_slots]
    loads = fetches(wide_in, own_wi.at[0:5, 0:wide_slots], own_wide, 0)
    loads += fetches(fine_in, own_i, own_floats, 4)
    for load in loads:
        load.start()
    for load in loads:
        load.wait()

    def lists():
        cells = own_i[...]
        level, radius = cells[0:1], cells[1:2]
        row_tile, col_tile = halved(row_tiles[0], level), halved(col_tiles[0], level)
        row, col = cells[2:3] - brick * row_tile, cells[3:4] - column * col_tile
        bounds = (row_tile, col_tile, row - radius, row + radius, col - radius, col + radius)
        keep = [
            jnp.where(touched(up, across, *bounds) & when_brick(up), 1.0, 0.0)
            for up, across in DIRECTIONS
        ]
        keep = jnp.concatenate(keep, 0)
        at = jnp.where(keep > 0.0, ranks(keep, True), -1.0)
        caps = by_line(CAPS, at.shape)
        lost = jnp.max(jnp.where(at >= caps, 1.0, 0.0))
        order = sorted(range(8), key=lambda d: STARTS[d])
        chosen = []
        for d in order:
            shape = (CAPS[d], slots)
            chosen.append(jnp.where(at[d : d + 1] == iota(shape).astype(F32), 1.0, 0.0))
        used = sum(CAPS)
        chosen.append(jnp.zeros((LISTS - used, slots), F32))
        found = gather(cells, own_floats[0:FLOATS, :], jnp.concatenate(chosen, 0).astype(BF16))
        list_i[...] = found[0:8].astype(I32)
        list_f[0:FLOATS] = found[5 : 5 + FLOATS]
        own_wi[5:8, 0:wide_slots] = jnp.broadcast_to(lost, (3, wide_slots)).astype(I32)

    lists()
    wide_i[:, mine] = own_wi[:, 0:wide_slots]
    wide_f[:, mine] = own_wide[...]

    below = (brick > 0).astype(I32)
    above = (brick < bricks - 1).astype(I32)
    pl.semaphore_wait(barrier, columns - 1 + columns * (below + above))

    def wide_copy(to_brick, to_column, k):
        other = to_brick * columns + to_column
        return pltpu.make_async_remote_copy(
            src_ref=(own_wi.at[:, 0:wide_slots], own_wide)[k],
            dst_ref=(wide_i, wide_f)[k].at[:, mine],
            send_sem=wide_send.at[other, k],
            recv_sem=wide_recv.at[me, k],
            device_id=place(to_brick, to_column),
            device_id_type=MESH,
        )

    def wide_to(to_brick, first):
        @pl.loop(first, columns)
        def _(step):
            for k in range(2):
                wide_copy(to_brick, at_column(step), k).start()

    def fine_copy(direction, k):
        up, across = DIRECTIONS[direction]
        slot = 7 - direction
        first, width = blocks(direction)
        return pltpu.make_async_remote_copy(
            src_ref=(list_i, list_f)[k].at[:, first : first + width],
            dst_ref=(near_i, near_f)[k].at[:, slot * 2 * LANES : slot * 2 * LANES + width],
            send_sem=fine_send.at[direction, k],
            recv_sem=fine_recv.at[slot, k],
            device_id=place(brick + up, at_column(across + columns)),
            device_id_type=MESH,
        )

    def token(step, sem):
        pl.semaphore_signal(sem, inc=1, device_id=place(brick + step, column), device_id_type=MESH)

    for step in (-1, 1):

        @pl.when(when_brick(step))
        def _():
            wide_to(brick + step, 0)

    wide_to(brick, 1)

    @pl.when(brick >= 2)
    def _():
        pl.semaphore_wait(up_sem, 1)

    @pl.when(jnp.logical_and(brick >= 1, brick < bricks - 1))
    def _():
        token(1, up_sem)

    @pl.when(jnp.logical_and(brick >= 1, brick == bricks - 2))
    def _():
        token(-1, down_sem)

    @pl.loop(0, jnp.maximum(brick - 1, 0))
    def _(to_brick):
        wide_to(to_brick, 0)

    for direction in (1, 6, 0, 2, 5, 7, 3, 4):

        @pl.when(when_brick(DIRECTIONS[direction][0]))
        def _():
            for k in range(2):
                fine_copy(direction, k).start()

    row0[...], row1[...], cols[...], depth[...] = fine_factors(
        own_i[...], own_floats[0:FLOATS, :], bricks, columns, brick, column
    )

    def slab(level, first, per):
        weights = jnp.concatenate(
            [
                (rows[level][pl.ds(first + i, 1), :] * cols[0 : col_tiles[level], :]).astype(BF16)
                for i in range(per)
            ],
            0,
        )
        result = product(weights, depth[0 : periods[level], :])
        return result.reshape(per, col_tiles[level], periods[level])

    per1 = min(16, row_tiles[1])
    per0 = min(16, row_tiles[0])

    @pl.loop(0, row_tiles[1] // per1)
    def _(i):
        parts[1][pl.ds(i * per1, per1)] = slab(1, i * per1, per1)

    def above_ready():
        @pl.when(brick < bricks - 2)
        def _():
            pl.semaphore_wait(down_sem, 1)

            @pl.when(brick >= 1)
            def _():
                token(-1, down_sem)

            @pl.loop(jnp.minimum(brick + 2, bricks), bricks)
            def _(to_brick):
                wide_to(to_brick, 0)

    @pl.when(brick >= 1)
    def _():
        above_ready()

    half0 = row_tiles[0] // per0 // 2

    @pl.loop(0, half0)
    def _(i):
        parts[0][pl.ds(i * per0, per0)] = slab(0, i * per0, per0)

    @pl.when(brick == 0)
    def _():
        above_ready()

    @pl.loop(half0, row_tiles[0] // per0)
    def _(i):
        parts[0][pl.ds(i * per0, per0)] = slab(0, i * per0, per0)

    for direction in range(8):

        @pl.when(when_brick(DIRECTIONS[direction][0]))
        def _():
            for k in range(2):
                fine_copy(direction, k).wait_send()
                fine_copy(7 - direction, k).wait_recv()

    def near_block(block):
        shape = (8, LANES)
        lane = lax.broadcasted_iota(I32, shape, 1) + block * LANES
        out_i, out_f = jnp.zeros(shape, I32), jnp.zeros(shape, F32)
        for d in range(8):
            first, width = blocks(d)
            if not first <= block * LANES < first + width:
                continue
            slot = 7 - d
            at = slot * 2 * LANES + block * LANES - first
            span = slice(at, at + LANES)
            valid = when_brick(-DIRECTIONS[d][0])
            inside = (lane >= STARTS[d]) & (lane < STARTS[d] + CAPS[d]) & valid
            out_i = jnp.where(inside, near_i[:, span], out_i)
            out_f = jnp.where(inside, near_f[:, span], out_f)
        return out_i, out_f

    pieces = [near_block(block) for block in range(LISTS // LANES)]
    row02[...], row12[...], cols2[...], depth2[...] = fine_factors(
        jnp.concatenate([a for a, b in pieces], 1),
        jnp.concatenate([b for a, b in pieces], 1),
        bricks,
        columns,
        brick,
        column,
    )
    add_spill(parts, (row02, row12), cols2, depth2, row_tiles, col_tiles, periods)

    @pl.loop(1, devices)
    def _(step):
        at = lax.rem(me + step, devices)
        spot = pl.ds(pl.multiple_of(at * wide_slots, wide_slots), wide_slots)
        for k in range(2):
            wide_copy(at // columns, lax.rem(at, columns), k).wait_send()
            ref = (wide_i, wide_f)[k].at[:, spot]
            own = (own_wi.at[:, 0:wide_slots], own_wide)[k]
            pltpu.make_async_copy(own, ref, wide_recv.at[at, k]).wait()

    over[0] = jnp.max(wide_i[5:6, :])


def blocks(direction):
    first = STARTS[direction] // LANES * LANES
    last = STARTS[direction] + CAPS[direction]
    return first, (last - first + LANES - 1) // LANES * LANES


def local_part(mesh_shape, fine, wide):
    bricks, reps, subs = (mesh_shape[name] for name in ("brick", "rep", "sub"))
    columns = reps * subs
    devices = bricks * columns
    row_tiles, col_tiles, periods = tiles(bricks, columns)
    slots, wide_slots = fine[0].shape[1], wide[0].shape[1]
    outs = [
        pltpu.VMEM((8, devices * wide_slots), I32),
        pltpu.VMEM((8, devices * wide_slots), F32),
    ] + [pltpu.VMEM((row_tiles[k], col_tiles[k], periods[k]), F32) for k in range(2)]
    outs += [jax.ShapeDtypeStruct((1,), I32)]
    return pl.pallas_call(
        functools.partial(local_kernel, bricks, reps, subs),
        out_shape=outs,
        in_specs=[pl.BlockSpec(memory_space=pltpu.HBM)] * 8,
        out_specs=[pl.BlockSpec(memory_space=pltpu.VMEM)] * 4
        + [pl.BlockSpec(memory_space=pltpu.SMEM)],
        scratch_shapes=[
            pltpu.VMEM((5, slots), I32),
            pltpu.VMEM((8, slots + 128), F32),
            pltpu.VMEM((8, wide_slots + 128), I32),
            pltpu.VMEM((8, wide_slots + 128), F32),
            pltpu.VMEM((periods[0], slots), BF16),
            pltpu.VMEM((col_tiles[0], slots), F32),
            pltpu.VMEM((row_tiles[0], slots), F32),
            pltpu.VMEM((row_tiles[1], slots), F32),
            pltpu.VMEM((8, LISTS), I32),
            pltpu.VMEM((8, LISTS), F32),
            pltpu.VMEM((8, 16 * LANES), I32),
            pltpu.VMEM((8, 16 * LANES), F32),
            pltpu.VMEM((periods[0], LISTS), BF16),
            pltpu.VMEM((col_tiles[0], LISTS), F32),
            pltpu.VMEM((row_tiles[0], LISTS), F32),
            pltpu.VMEM((row_tiles[1], LISTS), F32),
            pltpu.SemaphoreType.DMA((8, 2)),
            pltpu.SemaphoreType.DMA((8, 2)),
            pltpu.SemaphoreType.DMA((devices, 2)),
            pltpu.SemaphoreType.DMA((devices, 2)),
            pltpu.SemaphoreType.DMA((8,)),
            pltpu.SemaphoreType.REGULAR,
            pltpu.SemaphoreType.REGULAR,
        ],
        compiler_params=pltpu.CompilerParams(
            collective_id=0, has_side_effects=True, vmem_limit_bytes=30 * 1024 * 1024
        ),
        name="local_part",
    )(*[pltpu.with_memory_space_constraint(a, pltpu.HBM) for a in (*fine, *wide)])


def exchange_kernel(bricks, reps, subs, *refs):
    ins, outs = refs[0:4], refs[4:8]
    send, recv = refs[8:]
    columns = reps * subs
    brick = lax.axis_index("brick")
    column = lax.axis_index("rep") * subs + lax.axis_index("sub")
    slots = ins[0].shape[1]

    def place(direction):
        up, across = DIRECTIONS[direction]
        at = lax.rem(column + across + columns, columns)
        return {"brick": brick + up, "rep": at // subs, "sub": at % subs}

    def exists(direction):
        up = DIRECTIONS[direction][0]
        return jnp.logical_and(brick + up >= 0, brick + up < bricks)

    barrier = pltpu.get_barrier_semaphore()
    for direction in range(8):

        @pl.when(exists(direction))
        def _():
            pl.semaphore_signal(barrier, inc=1, device_id=place(direction), device_id_type=MESH)

    below = (brick > 0).astype(I32)
    above = (brick < bricks - 1).astype(I32)
    pl.semaphore_wait(barrier, 2 + 3 * (below + above))

    def copy(direction, k):
        slot = 7 - direction
        return pltpu.make_async_remote_copy(
            src_ref=ins[k],
            dst_ref=outs[k].at[:, pl.ds(slot * slots, slots)],
            send_sem=send.at[direction, k],
            recv_sem=recv.at[slot, k],
            device_id=place(direction),
            device_id_type=MESH,
        )

    for direction in range(8):

        @pl.when(exists(direction))
        def _():
            for k in range(4):
                copy(direction, k).start()

    for direction in range(8):

        @pl.when(exists(direction))
        def _():
            for k in range(4):
                copy(direction, k).wait_send()
                copy(7 - direction, k).wait_recv()


def exchange(mesh_shape, *fine):
    bricks, reps, subs = (mesh_shape[name] for name in ("brick", "rep", "sub"))
    vmem = pl.BlockSpec(memory_space=pltpu.VMEM)
    return pl.pallas_call(
        functools.partial(exchange_kernel, bricks, reps, subs),
        out_shape=[jax.ShapeDtypeStruct((a.shape[0], 8 * a.shape[1]), a.dtype) for a in fine],
        in_specs=[vmem] * 4,
        out_specs=[vmem] * 4,
        scratch_shapes=[pltpu.SemaphoreType.DMA((8, 4)), pltpu.SemaphoreType.DMA((8, 4))],
        compiler_params=pltpu.CompilerParams(
            collective_id=1, has_side_effects=True, vmem_limit_bytes=20 * 1024 * 1024
        ),
        name="exchange",
    )(*fine)


def repair_kernel(bricks, columns, subs, slots, *refs):
    near_i, exponent, charge, offset, grid0, grid1, out0, out1 = refs[0:8]
    part0, part1, depth, cols, row0, row1, spread_at, chunks, sems = refs[8:]
    brick = lax.axis_index("brick")
    column = lax.axis_index("rep") * subs + lax.axis_index("sub")
    row_tiles, col_tiles, periods = tiles(bricks, columns)
    parts, outs, rows = (part0, part1), (out0, out1), (row0, row1)
    loads = [pltpu.make_async_copy(outs[k], parts[k], sems.at[k]) for k in range(2)]
    for load in loads:
        load.start()
    for load in loads:
        load.wait()

    def near_table(span):
        return near_i[:, span], jnp.concatenate([offset[:, span], exponent[:, span], charge[:, span]], 0)

    def gather_spill(chunk):
        total = jnp.zeros((16, SPILL), F32)
        at = iota((SPILL, slots)).astype(F32) + (chunk * SPILL).astype(F32)
        for s in range(8):
            where_to = spread_at[s : s + 1, :]
            cells, floats = near_table(pl.ds(s * slots, slots))
            cells = jnp.where(where_to >= 0, cells, 0)
            floats = jnp.where(where_to >= 0, floats, 0.0)
            total += gather(cells, floats, jnp.where(where_to == at, 1.0, 0.0).astype(BF16))
        return total[0:8].astype(I32), total[5 : 5 + FLOATS]

    def spill_places():
        def lined(k):
            return jnp.concatenate(
                [near_i[k : k + 1, s * slots : (s + 1) * slots] for s in range(8)], 0
            )

        level, radius, c0, c1 = (lined(k) for k in range(4))
        first = level == 0
        row_tile = jnp.where(first, row_tiles[0], row_tiles[1])
        col_tile = jnp.where(first, col_tiles[0], col_tiles[1])
        keep = []
        for s in range(8):
            up, across = DIRECTIONS[7 - s]
            own = slice(s, s + 1)
            row = c0[own] - (brick - up) * row_tile[own]
            col = c1[own] - lax.rem(column - across + columns, columns) * col_tile[own]
            reach = radius[own]
            bounds = (row_tile[own], col_tile[own], row - reach, row + reach, col - reach, col + reach)
            valid = (brick - up >= 0) & (brick - up < bricks)
            keep.append(jnp.where(touched(up, across, *bounds) & valid, 1.0, 0.0))
        keep = jnp.concatenate(keep, 0)
        caps = by_line(CAPS[::-1], keep.shape)
        keep = jnp.where((keep > 0.0) & (ranks(keep, True) >= caps), 1.0, 0.0)
        at = jnp.where(keep > 0.0, ranks(keep, False), -1.0)
        spread_at[...] = at
        chunks[0] = (jnp.max(at).astype(I32) + SPILL) // SPILL

    spill_places()

    @pl.loop(0, chunks[0])
    def _(chunk):
        cells, floats = gather_spill(chunk)
        row0[...], row1[...], cols[...], depth[...] = fine_factors(
            cells, floats, bricks, columns, brick, column
        )
        add_spill(parts, rows, cols, depth, row_tiles, col_tiles, periods)

    copies = [pltpu.make_async_copy(parts[k], outs[k], sems.at[k]) for k in range(2)]
    for copy in copies:
        copy.start()
    for copy in copies:
        copy.wait()


def repair(mesh_shape, near, grids):
    bricks, reps, subs = (mesh_shape[name] for name in ("brick", "rep", "sub"))
    columns = reps * subs
    row_tiles, col_tiles, periods = tiles(bricks, columns)
    slots = near[0].shape[1] // 8
    vmem, anywhere = pl.BlockSpec(memory_space=pltpu.VMEM), pl.BlockSpec(memory_space=pltpu.HBM)
    return pl.pallas_call(
        functools.partial(repair_kernel, bricks, columns, subs, slots),
        out_shape=[pltpu.HBM(a.shape, a.dtype) for a in grids],
        in_specs=[vmem] * 4 + [anywhere] * 2,
        out_specs=[anywhere] * 2,
        input_output_aliases={4: 0, 5: 1},
        scratch_shapes=[pltpu.VMEM(a.shape, a.dtype) for a in grids]
        + [
            pltpu.VMEM((periods[0], SPILL), BF16),
            pltpu.VMEM((col_tiles[0], SPILL), F32),
            pltpu.VMEM((row_tiles[0], SPILL), F32),
            pltpu.VMEM((row_tiles[1], SPILL), F32),
            pltpu.VMEM((8, slots), F32),
            pltpu.SMEM((1,), I32),
            pltpu.SemaphoreType.DMA((2,)),
        ],
        compiler_params=pltpu.CompilerParams(vmem_limit_bytes=40 * 1024 * 1024),
        name="repair",
    )(*near, *grids)


def finish_kernel(bricks, wide_block, *refs):
    wide_i, wide_f, part0, part1 = refs[0:4]
    out0, out1, out2, out3, out4, sems = refs[4:]
    brick = lax.axis_index("brick")
    parts, outs = (part0, part1), (out0, out1)
    copies = [pltpu.make_async_copy(parts[k], outs[k], sems.at[k]) for k in range(2)]
    for copy in copies:
        copy.start()

    def wide_part(part):
        span = pl.ds(pl.multiple_of(part * wide_block, wide_block), wide_block)
        cells, floats = wide_i[:, span], wide_f[0:FLOATS, span]
        share = (GRID >> 2) // bricks
        which = cells[0:1]
        row_weight = row_factor(cells, floats, ROWS >> 2, ROWS, 0)
        col = column_factor(cells, floats, share, GRID // bricks, brick)
        lanes = GRID >> 2
        depth_value = depth_factor(cells, floats, lanes)
        for level, out in ((2, out2), (3, out3), (4, out4)):
            period = GRID >> level
            height = ROWS >> level
            share = period // bricks
            group = min(share, 8)
            copies = lanes // period
            width = min(copies, group)
            own = jnp.where(which == level, row_weight[0:height], 0.0)
            lane = lax.broadcasted_iota(I32, (height, lanes), 1) // period
            for first in range(0, share, group):
                weights = jnp.concatenate(
                    [(own * col[i : i + 1]).astype(BF16) for i in range(first, first + group)], 0
                )
                result = product(weights, depth_value)
                for i in range(0, group, width):
                    piece = result[i * height : (i + 1) * height]
                    for j in range(1, width):
                        piece = jnp.where(
                            lane == j, result[(i + j) * height : (i + j + 1) * height], piece
                        )
                    start = (first + i) * period
                    out[:, start : start + width * period] += piece[:, 0 : width * period]

    for ref in (out2, out3, out4):
        ref[...] = jnp.zeros(ref.shape, F32)

    @pl.loop(0, wide_i.shape[1] // wide_block)
    def _(part):
        wide_part(part)

    for copy in copies:
        copy.wait()


def finish(mesh_shape, got):
    bricks, reps, subs = (mesh_shape[name] for name in ("brick", "rep", "sub"))
    columns = reps * subs
    row_tiles, col_tiles, periods = tiles(bricks, columns)
    block = min(WIDE_BLOCK, got[0].shape[1])
    shapes = [(row_tiles[level], col_tiles[level], periods[level]) for level in range(2)]
    shapes += [(ROWS >> level, (GRID >> level) ** 2 // bricks) for level in (2, 3, 4)]
    vmem, anywhere = pl.BlockSpec(memory_space=pltpu.VMEM), pl.BlockSpec(memory_space=pltpu.HBM)
    return pl.pallas_call(
        functools.partial(finish_kernel, bricks, block),
        out_shape=[pltpu.HBM(shape, F32) for shape in shapes[:2]]
        + [jax.ShapeDtypeStruct(shape, F32) for shape in shapes[2:]],
        in_specs=[vmem] * 4,
        out_specs=[anywhere] * 2 + [vmem] * 3,
        scratch_shapes=[pltpu.SemaphoreType.DMA((2,))],
        compiler_params=pltpu.CompilerParams(vmem_limit_bytes=30 * 1024 * 1024),
        name="finish",
    )(*got[0:4])


def solution(mesh):
    shape = dict(mesh.shape)

    def per_device(
        fine_cells,
        fine_exponent,
        fine_charge,
        fine_offset,
        wide_cells,
        wide_exponent,
        wide_charge,
        wide_offset,
    ):
        fine = (fine_cells, fine_exponent[None, :], fine_charge[None, :], fine_offset)
        wide = (wide_cells, wide_exponent[None, :], wide_charge[None, :], wide_offset)
        got = local_part(shape, fine, wide)
        outs = finish(shape, got)

        def mend(state):
            near = exchange(shape, *fine)
            return (jnp.zeros((), I32), *repair(shape, near, state[1:]))

        state = lax.while_loop(lambda state: state[0] > 0, mend, (got[4][0], *outs[0:2]))
        return (*state[1:], *outs[2:])

    split = P(("parts", "brick", "rep", "sub"))
    table = P(None, ("parts", "brick", "rep", "sub"))
    return jax.shard_map(
        per_device,
        mesh=mesh,
        in_specs=(table, split, split, table, table, split, split, table),
        out_specs=(
            P(("parts", "brick"), ("rep", "sub"), None),
            P(("parts", "brick"), ("rep", "sub"), None),
            P("parts", "brick"),
            P("parts", "brick"),
            P("parts", "brick"),
        ),
        check_vma=False,
    )
```

```python
import functools
import math

import jax
import jax.numpy as jnp
from jax import lax
from jax.experimental import pallas as pl
from jax.experimental.pallas import tpu as pltpu
from jax.sharding import PartitionSpec as P

GRID = 512
ROWS = 128
HALF = 4
SPILL = 256
WIDE_BLOCK = 1024
DIRECTIONS = [(i, j) for i in (-1, 0, 1) for j in (-1, 0, 1) if (i, j) != (0, 0)]
MESH = pl.DeviceIdType.MESH
F32 = jnp.float32
BF16 = jnp.bfloat16
I32 = jnp.int32
LOG2E = math.log2(math.e)
FLOATS = 5
LISTS = 512
CAPS = (16, 160, 16, 48, 48, 16, 160, 16)
STARTS = (320, 160, 336, 384, 432, 352, 0, 368)
LANES = 128


def factor(cells, centre, radius, exponent, shift, period=None):
    reach = cells - (centre - radius)
    if period is not None:
        reach = reach & (period - 1)
        inside = reach <= 2 * radius
    else:
        inside = (reach >= 0) & (reach <= 2 * radius)
    spread = reach.astype(F32) - (radius.astype(F32) + shift)
    return jnp.where(inside, jnp.exp2((exponent * -LOG2E) * (spread * spread)), 0.0)


def halved(size, level):
    return lax.shift_right_logical(jnp.full(level.shape, size, I32), level)


def product(left, right):
    return lax.dot_general(left, right, (((1,), (1,)), ((), ())), preferred_element_type=F32)


def iota(shape):
    return lax.broadcasted_iota(I32, shape, 0)


def row_factor(cells, floats, rows, row_tile, row_block):
    level, radius = cells[0:1], cells[1:2]
    centre = cells[2:3] - row_block * halved(row_tile, level)
    shape = (rows, cells.shape[1])
    return floats[4:5] * factor(iota(shape), centre, radius, floats[3:4], floats[0:1])


def column_factor(cells, floats, columns, col_tile, col_block):
    level, radius = cells[0:1], cells[1:2]
    centre = cells[3:4] - col_block * halved(col_tile, level)
    shape = (columns, cells.shape[1])
    return factor(iota(shape), centre, radius, floats[3:4], floats[1:2], halved(GRID, level))


def depth_factor(cells, floats, width):
    level, radius = cells[0:1], cells[1:2]
    shape = (width, cells.shape[1])
    return factor(
        iota(shape), cells[4:5], radius, floats[3:4], floats[2:3], halved(GRID, level)
    ).astype(BF16)


def tiles(bricks, columns):
    row_tiles = [(ROWS >> level) // bricks for level in range(2)]
    col_tiles = [(GRID >> level) // columns for level in range(2)]
    periods = [GRID >> level for level in range(2)]
    return row_tiles, col_tiles, periods


def fine_factors(cells, floats, bricks, columns, brick, column):
    row_tiles, col_tiles, periods = tiles(bricks, columns)
    level = cells[0:1]
    row_weight = row_factor(cells, floats, row_tiles[0], row_tiles[0], brick)
    first = jnp.where(level == 0, row_weight, 0.0)
    second = jnp.where(level == 1, row_weight[0 : row_tiles[1]], 0.0)
    col = column_factor(cells, floats, col_tiles[0], col_tiles[0], column)
    return first, second, col, depth_factor(cells, floats, periods[0])


def ranks(keep, by_row):
    count = keep.shape[1] // LANES
    piled = jnp.concatenate([keep[:, i * LANES : (i + 1) * LANES] for i in range(count)], 0)
    height = piled.shape[0]
    square = (LANES, LANES)
    upper = iota(square) <= lax.broadcasted_iota(I32, square, 1)
    within = jnp.dot(
        piled.astype(BF16), jnp.where(upper, 1.0, 0.0).astype(BF16), preferred_element_type=F32
    )
    sums = jnp.broadcast_to(within[:, LANES - 1 : LANES], piled.shape)
    square = (height, height)
    gap = iota(square) - lax.broadcasted_iota(I32, square, 1)
    lower = gap > 0
    if by_row:
        lower &= (gap & 7) == 0
    before = jnp.dot(
        jnp.where(lower, 1.0, 0.0).astype(BF16), sums.astype(BF16), preferred_element_type=F32
    )
    at = before + within - 1.0
    return jnp.concatenate([at[i * 8 : (i + 1) * 8] for i in range(count)], 1)


def gather(cells, floats, chosen):
    count = cells.shape[1]
    pad = jnp.zeros((16 - 5 - FLOATS, count), F32)
    values = jnp.concatenate([cells.astype(F32), floats, pad], 0)
    high = values.astype(BF16)
    rest = values - high.astype(F32)
    middle = rest.astype(BF16)
    low = (rest - middle.astype(F32)).astype(BF16)
    found = product(jnp.concatenate([high, middle, low], 0), chosen)
    return found[0:16] + found[16:32] + found[32:48]


def by_line(values, shape):
    line = iota(shape)
    out = jnp.full(shape, values[0], F32)
    for k in range(1, len(values)):
        out = jnp.where(line == k, float(values[k]), out)
    return out


def touched(up, across, row_tile, col_tile, low0, high0, low1, high1):
    along0 = {-1: low0 < 0, 0: None, 1: high0 >= row_tile}[up]
    along1 = {-1: low1 < 0, 0: None, 1: high1 >= col_tile}[across]
    if along0 is None:
        return along1
    return along0 if along1 is None else along0 & along1


def add_spill(parts, rows, cols, depth, row_tiles, col_tiles, periods):
    edge = 2 * HALF

    def add_rows(level, row, height, col, width):
        weights = jnp.concatenate(
            [
                (rows[level][row + i : row + i + 1, :] * cols[col : col + width, :]).astype(BF16)
                for i in range(height)
            ],
            0,
        )
        result = product(weights, depth[0 : periods[level], :])
        spot = (slice(row, row + height), slice(col, col + width))
        parts[level][spot] += result.reshape(height, width, periods[level])

    for level in range(2):
        tall, wide = row_tiles[level], col_tiles[level]
        if tall > 2 * HALF and wide > 2 * edge:
            for row in (0, tall - HALF):
                add_rows(level, row, HALF, 0, wide)
            for col in (0, wide - edge):
                add_rows(level, HALF, tall - 2 * HALF, col, edge)
        else:
            for row in range(0, tall, HALF):
                add_rows(level, row, min(HALF, tall - row), 0, wide)


def local_kernel(bricks, reps, subs, *refs):
    fine_in, wide_in = refs[0:4], refs[4:8]
    wide_i, wide_f, part0, part1, over = refs[8:13]
    own_i, own_f, own_wi, own_wf, depth, cols, row0, row1 = refs[13:21]
    list_i, list_f, near_i, near_f, depth2, cols2, row02, row12 = refs[21:29]
    fine_send, fine_recv, wide_send, wide_recv, own_sem = refs[29:]
    columns = reps * subs
    devices = bricks * columns
    brick = lax.axis_index("brick")
    column = lax.axis_index("rep") * subs + lax.axis_index("sub")
    me = brick * columns + column
    slots = own_i.shape[1]
    own_floats = own_f.at[:, 0:slots]
    wide_slots = wide_in[0].shape[1]
    row_tiles, col_tiles, periods = tiles(bricks, columns)
    parts = (part0, part1)
    rows = (row0, row1)

    rep_at, sub_at = lax.axis_index("rep"), lax.axis_index("sub")
    sides = {0: (rep_at, sub_at)}
    for across in (-1, 1):
        at = lax.rem(column + across + columns, columns)
        sides[across] = (lax.div(at, subs), lax.rem(at, subs))

    def place(at_brick, at_rep, at_sub):
        return {"brick": at_brick, "rep": at_rep, "sub": at_sub}

    def each_column(at_brick, act):
        for k in range(columns):

            @pl.when(at_brick * columns + k != me)
            def _():
                act(at_brick, k)

    def when_brick(step):
        return jnp.logical_and(brick + step >= 0, brick + step < bricks)

    barrier = pltpu.get_barrier_semaphore()

    def greet(at_brick, k):
        where = place(at_brick, k // subs, k % subs)
        pl.semaphore_signal(barrier, inc=1, device_id=where, device_id_type=MESH)

    @pl.loop(0, bricks)
    def _(at_brick):
        each_column(at_brick, greet)

    mine = pl.ds(pl.multiple_of(me * wide_slots, wide_slots), wide_slots)

    def fetches(source, whole_i, whole_f, first):
        pairs = [
            (source[0], whole_i),
            (source[3], whole_f.at[0:3]),
            (source[1], whole_f.at[3:4]),
            (source[2], whole_f.at[4:5]),
        ]
        return [
            pltpu.make_async_copy(a, b, own_sem.at[first + k]) for k, (a, b) in enumerate(pairs)
        ]

    own_wide = own_wf.at[:, 0:wide_slots]
    loads = fetches(wide_in, own_wi.at[0:5, 0:wide_slots], own_wide, 0)
    loads += fetches(fine_in, own_i, own_floats, 4)
    for load in loads:
        load.start()
    for load in loads:
        load.wait()

    def lists():
        cells = own_i[...]
        level, radius = cells[0:1], cells[1:2]
        row_tile, col_tile = halved(row_tiles[0], level), halved(col_tiles[0], level)
        row, col = cells[2:3] - brick * row_tile, cells[3:4] - column * col_tile
        bounds = (row_tile, col_tile, row - radius, row + radius, col - radius, col + radius)
        keep = [
            jnp.where(touched(up, across, *bounds) & when_brick(up), 1.0, 0.0)
            for up, across in DIRECTIONS
        ]
        keep = jnp.concatenate(keep, 0)
        at = jnp.where(keep > 0.0, ranks(keep, True), -1.0)
        caps = by_line(CAPS, at.shape)
        lost = jnp.max(jnp.where(at >= caps, 1.0, 0.0))
        order = sorted(range(8), key=lambda d: STARTS[d])
        chosen = []
        for d in order:
            shape = (CAPS[d], slots)
            chosen.append(jnp.where(at[d : d + 1] == iota(shape).astype(F32), 1.0, 0.0))
        used = sum(CAPS)
        chosen.append(jnp.zeros((LISTS - used, slots), F32))
        found = gather(cells, own_floats[0:FLOATS, :], jnp.concatenate(chosen, 0).astype(BF16))
        list_i[...] = found[0:8].astype(I32)
        list_f[0:FLOATS] = found[5 : 5 + FLOATS]
        own_wi[5:8, 0:wide_slots] = jnp.broadcast_to(lost, (3, wide_slots)).astype(I32)

    lists()
    wide_i[:, mine] = own_wi[:, 0:wide_slots]
    wide_f[:, mine] = own_wide[...]

    def wide_copy(to_brick, to_column, k):
        other = to_brick * columns + to_column
        return pltpu.make_async_remote_copy(
            src_ref=(own_wi.at[:, 0:wide_slots], own_wide)[k],
            dst_ref=(wide_i, wide_f)[k].at[:, mine],
            send_sem=wide_send.at[other, k],
            recv_sem=wide_recv.at[me, k],
            device_id=place(to_brick, to_column // subs, to_column % subs),
            device_id_type=MESH,
        )

    def wide_to(to_brick):
        def start(at_brick, column_at):
            for k in range(2):
                wide_copy(at_brick, column_at, k).start()

        each_column(to_brick, start)

    def fine_copy(direction, k):
        up, across = DIRECTIONS[direction]
        slot = 7 - direction
        first, width = blocks(direction)
        return pltpu.make_async_remote_copy(
            src_ref=(list_i, list_f)[k].at[:, first : first + width],
            dst_ref=(near_i, near_f)[k].at[:, slot * 2 * LANES : slot * 2 * LANES + width],
            send_sem=fine_send.at[direction, k],
            recv_sem=fine_recv.at[slot, k],
            device_id=place(brick + up, *sides[across]),
            device_id_type=MESH,
        )

    def slab(level, first, per):
        weights = jnp.concatenate(
            [
                (rows[level][pl.ds(first + i, 1), :] * cols[0 : col_tiles[level], :]).astype(BF16)
                for i in range(per)
            ],
            0,
        )
        result = product(weights, depth[0 : periods[level], :])
        parts[level][pl.ds(first, per)] = result.reshape(per, col_tiles[level], periods[level])

    def send():
        pl.semaphore_wait(barrier, devices - 1)

        @pl.loop(0, brick)
        def _(to_brick):
            wide_to(to_brick)

        for direction in (1, 6, 0, 2, 5, 7, 3, 4):

            @pl.when(when_brick(DIRECTIONS[direction][0]))
            def _():
                for k in range(2):
                    fine_copy(direction, k).start()

        wide_to(brick)

        @pl.loop(brick + 1, bricks)
        def _(to_brick):
            wide_to(to_brick)

    per1 = min(16, row_tiles[1])
    per0 = min(16, row_tiles[0])
    halves = row_tiles[0] // per0
    gate = jnp.minimum((bricks - brick) // 2, halves + 1)

    @pl.loop(0, halves + 2)
    def _(stage):
        @pl.when(stage == gate)
        def _():
            send()

        @pl.when(stage == 0)
        def _():
            row0[...], row1[...], cols[...], depth[...] = fine_factors(
                own_i[...], own_floats[0:FLOATS, :], bricks, columns, brick, column
            )
            for i in range(row_tiles[1] // per1):
                slab(1, i * per1, per1)

        for half in range(halves):

            @pl.when(stage == half + 1)
            def _():
                slab(0, half * per0, per0)

    for direction in range(8):

        @pl.when(when_brick(DIRECTIONS[direction][0]))
        def _():
            for k in range(2):
                fine_copy(direction, k).wait_send()
                fine_copy(7 - direction, k).wait_recv()

    def near_block(block):
        shape = (8, LANES)
        lane = lax.broadcasted_iota(I32, shape, 1) + block * LANES
        out_i, out_f = jnp.zeros(shape, I32), jnp.zeros(shape, F32)
        for d in range(8):
            first, width = blocks(d)
            if not first <= block * LANES < first + width:
                continue
            slot = 7 - d
            at = slot * 2 * LANES + block * LANES - first
            span = slice(at, at + LANES)
            valid = when_brick(-DIRECTIONS[d][0])
            inside = (lane >= STARTS[d]) & (lane < STARTS[d] + CAPS[d]) & valid
            out_i = jnp.where(inside, near_i[:, span], out_i)
            out_f = jnp.where(inside, near_f[:, span], out_f)
        return out_i, out_f

    pieces = [near_block(block) for block in range(LISTS // LANES)]
    row02[...], row12[...], cols2[...], depth2[...] = fine_factors(
        jnp.concatenate([a for a, b in pieces], 1),
        jnp.concatenate([b for a, b in pieces], 1),
        bricks,
        columns,
        brick,
        column,
    )
    add_spill(parts, (row02, row12), cols2, depth2, row_tiles, col_tiles, periods)

    def arrive(at_brick, column_at):
        at = at_brick * columns + column_at
        spot = pl.ds(pl.multiple_of(at * wide_slots, wide_slots), wide_slots)
        for k in range(2):
            wide_copy(at_brick, column_at, k).wait_send()
            ref = (wide_i, wide_f)[k].at[:, spot]
            own = (own_wi.at[:, 0:wide_slots], own_wide)[k]
            pltpu.make_async_copy(own, ref, wide_recv.at[at, k]).wait()

    @pl.loop(0, bricks)
    def _(at_brick):
        each_column(at_brick, arrive)

    over[0] = jnp.max(wide_i[5:6, :])


def blocks(direction):
    first = STARTS[direction] // LANES * LANES
    last = STARTS[direction] + CAPS[direction]
    return first, (last - first + LANES - 1) // LANES * LANES


def local_part(mesh_shape, fine, wide):
    bricks, reps, subs = (mesh_shape[name] for name in ("brick", "rep", "sub"))
    columns = reps * subs
    devices = bricks * columns
    row_tiles, col_tiles, periods = tiles(bricks, columns)
    slots, wide_slots = fine[0].shape[1], wide[0].shape[1]
    outs = [
        pltpu.VMEM((8, devices * wide_slots), I32),
        pltpu.VMEM((8, devices * wide_slots), F32),
    ] + [pltpu.VMEM((row_tiles[k], col_tiles[k], periods[k]), F32) for k in range(2)]
    outs += [jax.ShapeDtypeStruct((1,), I32)]
    return pl.pallas_call(
        functools.partial(local_kernel, bricks, reps, subs),
        out_shape=outs,
        in_specs=[pl.BlockSpec(memory_space=pltpu.HBM)] * 8,
        out_specs=[pl.BlockSpec(memory_space=pltpu.VMEM)] * 4
        + [pl.BlockSpec(memory_space=pltpu.SMEM)],
        scratch_shapes=[
            pltpu.VMEM((5, slots), I32),
            pltpu.VMEM((8, slots + 128), F32),
            pltpu.VMEM((8, wide_slots + 128), I32),
            pltpu.VMEM((8, wide_slots + 128), F32),
            pltpu.VMEM((periods[0], slots), BF16),
            pltpu.VMEM((col_tiles[0], slots), F32),
            pltpu.VMEM((row_tiles[0], slots), F32),
            pltpu.VMEM((row_tiles[1], slots), F32),
            pltpu.VMEM((8, LISTS), I32),
            pltpu.VMEM((8, LISTS), F32),
            pltpu.VMEM((8, 16 * LANES), I32),
            pltpu.VMEM((8, 16 * LANES), F32),
            pltpu.VMEM((periods[0], LISTS), BF16),
            pltpu.VMEM((col_tiles[0], LISTS), F32),
            pltpu.VMEM((row_tiles[0], LISTS), F32),
            pltpu.VMEM((row_tiles[1], LISTS), F32),
            pltpu.SemaphoreType.DMA((8, 2)),
            pltpu.SemaphoreType.DMA((8, 2)),
            pltpu.SemaphoreType.DMA((devices, 2)),
            pltpu.SemaphoreType.DMA((devices, 2)),
            pltpu.SemaphoreType.DMA((8,)),
        ],
        compiler_params=pltpu.CompilerParams(
            collective_id=0, has_side_effects=True, vmem_limit_bytes=30 * 1024 * 1024
        ),
        name="local_part",
    )(*[pltpu.with_memory_space_constraint(a, pltpu.HBM) for a in (*fine, *wide)])


def exchange_kernel(bricks, reps, subs, *refs):
    ins, outs = refs[0:4], refs[4:8]
    send, recv = refs[8:]
    columns = reps * subs
    brick = lax.axis_index("brick")
    column = lax.axis_index("rep") * subs + lax.axis_index("sub")
    slots = ins[0].shape[1]

    def place(direction):
        up, across = DIRECTIONS[direction]
        at = lax.rem(column + across + columns, columns)
        return {"brick": brick + up, "rep": at // subs, "sub": at % subs}

    def exists(direction):
        up = DIRECTIONS[direction][0]
        return jnp.logical_and(brick + up >= 0, brick + up < bricks)

    barrier = pltpu.get_barrier_semaphore()
    for direction in range(8):

        @pl.when(exists(direction))
        def _():
            pl.semaphore_signal(barrier, inc=1, device_id=place(direction), device_id_type=MESH)

    below = (brick > 0).astype(I32)
    above = (brick < bricks - 1).astype(I32)
    pl.semaphore_wait(barrier, 2 + 3 * (below + above))

    def copy(direction, k):
        slot = 7 - direction
        return pltpu.make_async_remote_copy(
            src_ref=ins[k],
            dst_ref=outs[k].at[:, pl.ds(slot * slots, slots)],
            send_sem=send.at[direction, k],
            recv_sem=recv.at[slot, k],
            device_id=place(direction),
            device_id_type=MESH,
        )

    for direction in range(8):

        @pl.when(exists(direction))
        def _():
            for k in range(4):
                copy(direction, k).start()

    for direction in range(8):

        @pl.when(exists(direction))
        def _():
            for k in range(4):
                copy(direction, k).wait_send()
                copy(7 - direction, k).wait_recv()


def exchange(mesh_shape, *fine):
    bricks, reps, subs = (mesh_shape[name] for name in ("brick", "rep", "sub"))
    vmem = pl.BlockSpec(memory_space=pltpu.VMEM)
    return pl.pallas_call(
        functools.partial(exchange_kernel, bricks, reps, subs),
        out_shape=[jax.ShapeDtypeStruct((a.shape[0], 8 * a.shape[1]), a.dtype) for a in fine],
        in_specs=[vmem] * 4,
        out_specs=[vmem] * 4,
        scratch_shapes=[pltpu.SemaphoreType.DMA((8, 4)), pltpu.SemaphoreType.DMA((8, 4))],
        compiler_params=pltpu.CompilerParams(
            collective_id=1, has_side_effects=True, vmem_limit_bytes=20 * 1024 * 1024
        ),
        name="exchange",
    )(*fine)


def repair_kernel(bricks, columns, subs, slots, *refs):
    near_i, exponent, charge, offset, grid0, grid1, out0, out1 = refs[0:8]
    part0, part1, depth, cols, row0, row1, spread_at, chunks, sems = refs[8:]
    brick = lax.axis_index("brick")
    column = lax.axis_index("rep") * subs + lax.axis_index("sub")
    row_tiles, col_tiles, periods = tiles(bricks, columns)
    parts, outs, rows = (part0, part1), (out0, out1), (row0, row1)
    loads = [pltpu.make_async_copy(outs[k], parts[k], sems.at[k]) for k in range(2)]
    for load in loads:
        load.start()
    for load in loads:
        load.wait()

    def near_table(span):
        return near_i[:, span], jnp.concatenate([offset[:, span], exponent[:, span], charge[:, span]], 0)

    def gather_spill(chunk):
        total = jnp.zeros((16, SPILL), F32)
        at = iota((SPILL, slots)).astype(F32) + (chunk * SPILL).astype(F32)
        for s in range(8):
            where_to = spread_at[s : s + 1, :]
            cells, floats = near_table(pl.ds(s * slots, slots))
            cells = jnp.where(where_to >= 0, cells, 0)
            floats = jnp.where(where_to >= 0, floats, 0.0)
            total += gather(cells, floats, jnp.where(where_to == at, 1.0, 0.0).astype(BF16))
        return total[0:8].astype(I32), total[5 : 5 + FLOATS]

    def spill_places():
        def lined(k):
            return jnp.concatenate(
                [near_i[k : k + 1, s * slots : (s + 1) * slots] for s in range(8)], 0
            )

        level, radius, c0, c1 = (lined(k) for k in range(4))
        first = level == 0
        row_tile = jnp.where(first, row_tiles[0], row_tiles[1])
        col_tile = jnp.where(first, col_tiles[0], col_tiles[1])
        keep = []
        for s in range(8):
            up, across = DIRECTIONS[7 - s]
            own = slice(s, s + 1)
            row = c0[own] - (brick - up) * row_tile[own]
            col = c1[own] - lax.rem(column - across + columns, columns) * col_tile[own]
            reach = radius[own]
            bounds = (row_tile[own], col_tile[own], row - reach, row + reach, col - reach, col + reach)
            valid = (brick - up >= 0) & (brick - up < bricks)
            keep.append(jnp.where(touched(up, across, *bounds) & valid, 1.0, 0.0))
        keep = jnp.concatenate(keep, 0)
        caps = by_line(CAPS[::-1], keep.shape)
        keep = jnp.where((keep > 0.0) & (ranks(keep, True) >= caps), 1.0, 0.0)
        at = jnp.where(keep > 0.0, ranks(keep, False), -1.0)
        spread_at[...] = at
        chunks[0] = (jnp.max(at).astype(I32) + SPILL) // SPILL

    spill_places()

    @pl.loop(0, chunks[0])
    def _(chunk):
        cells, floats = gather_spill(chunk)
        row0[...], row1[...], cols[...], depth[...] = fine_factors(
            cells, floats, bricks, columns, brick, column
        )
        add_spill(parts, rows, cols, depth, row_tiles, col_tiles, periods)

    copies = [pltpu.make_async_copy(parts[k], outs[k], sems.at[k]) for k in range(2)]
    for copy in copies:
        copy.start()
    for copy in copies:
        copy.wait()


def repair(mesh_shape, near, grids):
    bricks, reps, subs = (mesh_shape[name] for name in ("brick", "rep", "sub"))
    columns = reps * subs
    row_tiles, col_tiles, periods = tiles(bricks, columns)
    slots = near[0].shape[1] // 8
    vmem, anywhere = pl.BlockSpec(memory_space=pltpu.VMEM), pl.BlockSpec(memory_space=pltpu.HBM)
    return pl.pallas_call(
        functools.partial(repair_kernel, bricks, columns, subs, slots),
        out_shape=[pltpu.HBM(a.shape, a.dtype) for a in grids],
        in_specs=[vmem] * 4 + [anywhere] * 2,
        out_specs=[anywhere] * 2,
        input_output_aliases={4: 0, 5: 1},
        scratch_shapes=[pltpu.VMEM(a.shape, a.dtype) for a in grids]
        + [
            pltpu.VMEM((periods[0], SPILL), BF16),
            pltpu.VMEM((col_tiles[0], SPILL), F32),
            pltpu.VMEM((row_tiles[0], SPILL), F32),
            pltpu.VMEM((row_tiles[1], SPILL), F32),
            pltpu.VMEM((8, slots), F32),
            pltpu.SMEM((1,), I32),
            pltpu.SemaphoreType.DMA((2,)),
        ],
        compiler_params=pltpu.CompilerParams(vmem_limit_bytes=40 * 1024 * 1024),
        name="repair",
    )(*near, *grids)


def finish_kernel(bricks, wide_block, *refs):
    wide_i, wide_f, part0, part1 = refs[0:4]
    out0, out1, out2, out3, out4, sems = refs[4:]
    brick = lax.axis_index("brick")
    parts, outs = (part0, part1), (out0, out1)
    copies = [pltpu.make_async_copy(parts[k], outs[k], sems.at[k]) for k in range(2)]
    for copy in copies:
        copy.start()

    def wide_part(part):
        span = pl.ds(pl.multiple_of(part * wide_block, wide_block), wide_block)
        cells, floats = wide_i[:, span], wide_f[0:FLOATS, span]
        share = (GRID >> 2) // bricks
        which = cells[0:1]
        row_weight = row_factor(cells, floats, ROWS >> 2, ROWS, 0)
        col = column_factor(cells, floats, share, GRID // bricks, brick)
        lanes = GRID >> 2
        depth_value = depth_factor(cells, floats, lanes)
        for level, out in ((2, out2), (3, out3), (4, out4)):
            period = GRID >> level
            height = ROWS >> level
            share = period // bricks
            group = min(share, 8)
            copies = lanes // period
            width = min(copies, group)
            own = jnp.where(which == level, row_weight[0:height], 0.0)
            lane = lax.broadcasted_iota(I32, (height, lanes), 1) // period
            for first in range(0, share, group):
                weights = jnp.concatenate(
                    [(own * col[i : i + 1]).astype(BF16) for i in range(first, first + group)], 0
                )
                result = product(weights, depth_value)
                for i in range(0, group, width):
                    piece = result[i * height : (i + 1) * height]
                    for j in range(1, width):
                        piece = jnp.where(
                            lane == j, result[(i + j) * height : (i + j + 1) * height], piece
                        )
                    start = (first + i) * period
                    out[:, start : start + width * period] += piece[:, 0 : width * period]

    for ref in (out2, out3, out4):
        ref[...] = jnp.zeros(ref.shape, F32)

    @pl.loop(0, wide_i.shape[1] // wide_block)
    def _(part):
        wide_part(part)

    for copy in copies:
        copy.wait()


def finish(mesh_shape, got):
    bricks, reps, subs = (mesh_shape[name] for name in ("brick", "rep", "sub"))
    columns = reps * subs
    row_tiles, col_tiles, periods = tiles(bricks, columns)
    block = min(WIDE_BLOCK, got[0].shape[1])
    shapes = [(row_tiles[level], col_tiles[level], periods[level]) for level in range(2)]
    shapes += [(ROWS >> level, (GRID >> level) ** 2 // bricks) for level in (2, 3, 4)]
    vmem, anywhere = pl.BlockSpec(memory_space=pltpu.VMEM), pl.BlockSpec(memory_space=pltpu.HBM)
    return pl.pallas_call(
        functools.partial(finish_kernel, bricks, block),
        out_shape=[pltpu.HBM(shape, F32) for shape in shapes[:2]]
        + [jax.ShapeDtypeStruct(shape, F32) for shape in shapes[2:]],
        in_specs=[vmem] * 4,
        out_specs=[anywhere] * 2 + [vmem] * 3,
        scratch_shapes=[pltpu.SemaphoreType.DMA((2,))],
        compiler_params=pltpu.CompilerParams(vmem_limit_bytes=30 * 1024 * 1024),
        name="finish",
    )(*got[0:4])


def solution(mesh):
    shape = dict(mesh.shape)

    def per_device(
        fine_cells,
        fine_exponent,
        fine_charge,
        fine_offset,
        wide_cells,
        wide_exponent,
        wide_charge,
        wide_offset,
    ):
        fine = (fine_cells, fine_exponent[None, :], fine_charge[None, :], fine_offset)
        wide = (wide_cells, wide_exponent[None, :], wide_charge[None, :], wide_offset)
        got = local_part(shape, fine, wide)
        outs = finish(shape, got)

        def mend(state):
            near = exchange(shape, *fine)
            return (jnp.zeros((), I32), *repair(shape, near, state[1:]))

        state = lax.while_loop(lambda state: state[0] > 0, mend, (got[4][0], *outs[0:2]))
        return (*state[1:], *outs[2:])

    split = P(("parts", "brick", "rep", "sub"))
    table = P(None, ("parts", "brick", "rep", "sub"))
    return jax.shard_map(
        per_device,
        mesh=mesh,
        in_specs=(table, split, split, table, table, split, split, table),
        out_specs=(
            P(("parts", "brick"), ("rep", "sub"), None),
            P(("parts", "brick"), ("rep", "sub"), None),
            P("parts", "brick"),
            P("parts", "brick"),
            P("parts", "brick"),
        ),
        check_vma=False,
    )
```
